128 devices in a mesh: south: 4 (over x), east: 8 (over y, core), down: 4 (over z).
Axes of the slice: x: 4, y: 4, z: 4, core: 2. Of those that a mesh axis runs over, the one named last changes fastest.
Arguments:
- field_now: float32 [32, 128, 512, 128], P('south', 'east', 'down'), may hold values from 0.2 to 1.8
- earlier: float32 [32, 128, 512, 128], P('south', 'east', 'down'), may hold values from 0.2 to 1.8
- speed_square: float32 [32, 128, 512, 128], P('south', 'east', 'down'), may hold values from 0.05 to 0.3
Outputs:
- running_total: float32 [32, 128, 512, 128], P('south', 'east', 'down')
- field_now_end: float32 [32, 128, 512, 128], P('south', 'east', 'down')
The draws below stay inside these ranges and needn't reach their ends.
All inputs are finite; a program needn't handle non-finite values.
Results may differ from the reference program's by a relative error of at most 0.00002.
Values sent between devices are 32-bit elements; how exact they have to be, the bound alone decides.
No kernel may reach another device: no remote copies, remote signals or barrier semaphores. Data moves between devices by JAX's collectives and lax.ppermute only.
A program may use at most 320 MiB of HBM per device.

```python
import jax
import jax.numpy as jnp
from jax import lax

GRID_J = 32
GRID_I = 128
GRID_K = 512
MEMBERS = 128
STEPS = 4


def levels(stream_key, shape, cuts, smallest, largest):
    loudness = 1.0
    for dim, blocks in cuts:
        draws = jax.random.uniform(jax.random.fold_in(jax.random.fold_in(stream_key, 6), dim), (blocks,), jnp.float32, smallest / len(cuts), largest / len(cuts))
        loudness = loudness * jnp.repeat(jnp.exp(draws), shape[dim] // blocks).reshape((-1,) + (1,) * (len(shape) - 1 - dim))
    return loudness


def setup_inputs(seed: int = 0) -> dict:
    key_list = jax.random.split(jax.random.key(seed), 4)
    field_now = jnp.clip(0.2 + 1.5999999 * jax.random.uniform(key_list[0], (GRID_J, GRID_I, GRID_K, MEMBERS), jnp.float32) ** levels(key_list[0], (GRID_J, GRID_I, GRID_K, MEMBERS), ((0, 4), (1, 8), (2, 4)), -0.2, 0.2), 0.2, 1.8)
    earlier = jnp.clip(0.2 + 1.5999999 * jax.random.uniform(key_list[1], (GRID_J, GRID_I, GRID_K, MEMBERS), jnp.float32) ** levels(key_list[1], (GRID_J, GRID_I, GRID_K, MEMBERS), ((0, 4), (1, 8), (2, 4)), -0.2, 0.2), 0.2, 1.8)
    speed_square = jnp.clip(0.05 + 0.25 * jax.random.uniform(key_list[2], (GRID_J, GRID_I, GRID_K, MEMBERS), jnp.float32) ** levels(key_list[2], (GRID_J, GRID_I, GRID_K, MEMBERS), ((0, 4), (1, 8), (2, 4)), -0.2, 0.2), 0.05, 0.3)
    return {"field_now": field_now, "earlier": earlier, "speed_square": speed_square}


def strip_edges(values, dims):
    for dim in dims:
        values = lax.slice_in_dim(values, 1, values.shape[dim] - 1, axis=dim)
    return values


def neighbour(values, dim, start, dims):
    others = [other for other in dims if other != dim]
    values = strip_edges(values, others)
    return lax.slice_in_dim(values, start, start + values.shape[dim] - 2, axis=dim)


def one_step(padded, before, speed_square):
    middle = strip_edges(padded, (0, 1, 2))
    lower = [neighbour(padded, dim, 0, (0, 1, 2)) for dim in (0, 1, 2)]
    upper = [neighbour(padded, dim, 2, (0, 1, 2)) for dim in (0, 1, 2)]
    spread = lower[0] + upper[0] + lower[1] + upper[1] + lower[2] + upper[2] - 6.0 * middle
    return 2.0 * middle - before + speed_square * spread


def reference(field_now, earlier, speed_square):
    for step in range(STEPS):
        later = one_step(jnp.pad(field_now, ((1, 1), (1, 1), (1, 1), (0, 0)), mode="constant"), earlier, speed_square)
        earlier, field_now = field_now, later
    running_total = jnp.cumsum(field_now, axis=0) / GRID_J
    return running_total, field_now
```

```python
import jax
import jax.numpy as jnp
from jax import lax
from jax.experimental import pallas as pl
from jax.experimental.pallas import tpu as pltpu
from jax.sharding import PartitionSpec as P


STEPS = 4
PAD = 8
ROWS = 32
MIB = 1 << 20


VM = pl.BlockSpec(memory_space=pltpu.VMEM)
HBM = pl.BlockSpec(memory_space=pltpu.HBM)


def call(body, ins, outs, out_specs, in_specs, alias=None, scratch=(), limit=6, flops=0, moved=0):
    return pl.pallas_call(
        body,
        out_shape=outs,
        in_specs=in_specs,
        out_specs=out_specs,
        scratch_shapes=scratch,
        input_output_aliases=alias or {},
        compiler_params=pltpu.CompilerParams(vmem_limit_bytes=limit * MIB),
        cost_estimate=pl.CostEstimate(flops=flops, bytes_accessed=moved, transcendentals=0),
    )(*ins)


def vmem(shape):
    return pltpu.VMEM(shape, jnp.float32)


def copy_all(copies):
    for copy in copies:
        copy.start()
    for copy in copies:
        copy.wait()


def ring(count, step):
    pairs = [(i, i + 1) for i in range(count - 1)]
    return pairs if step > 0 else [(b, a) for a, b in pairs]


def cell_rows(now, before, speed, j, i, k, jm, jp, im, ip):
    at = PAD + k
    mid = now[j, i, pl.ds(at, ROWS), :]
    spread = jm(k) + jp(k) + im(k) + ip(k)
    spread = spread + now[j, i, pl.ds(at - 1, ROWS), :] + now[j, i, pl.ds(at + 1, ROWS), :] - 6.0 * mid
    return 2.0 * mid - before[j, i, pl.ds(at, ROWS), :] + speed[j, i, pl.ds(k, ROWS), :] * spread


def inside(ref, j, i):
    return lambda k: ref[j, i, pl.ds(PAD + k, ROWS), :]


def face(ref, n):
    return lambda k: ref[n, pl.ds(k, ROWS), :]


def columns(now, before, speed, j, i, low_i, high_i, halo, put):
    jm, jp = halo
    for k in range(0, speed.shape[2], ROWS):
        new = cell_rows(now, before, speed, j, i, k, jm, jp, low_i, high_i)
        before[j, i, pl.ds(PAD + k, ROWS), :] = new
        for ref, n in put:
            ref[n, pl.ds(k, ROWS), :] = new


def solution(mesh):
    south, east, down = (mesh.shape[a] for a in ("south", "east", "down"))

    def shards(field_now, earlier, speed_square):
        nj, ni, nk, nm = field_now.shape
        half = ni // 2
        padded = (nj, ni, nk + 2 * PAD, nm)
        xs, ys, zs = (half, nk, nm), (nj, nk, nm), (nj, ni, nm)
        cells = half * nj * nk * nm

        def send(value, axis, count, step):
            return lax.ppermute(value, axis, ring(count, step))

        field_now, earlier, speed_square = (
            pltpu.with_memory_space_constraint(v, pltpu.HBM) for v in (field_now, earlier, speed_square)
        )

        def faces_body(field, xau, xad, xbu, xbd, yu, yd, sem):
            pairs = [
                (field.at[nj - 1, pl.ds(0, half)], xau),
                (field.at[0, pl.ds(0, half)], xad),
                (field.at[nj - 1, pl.ds(half, half)], xbu),
                (field.at[0, pl.ds(half, half)], xbd),
                (field.at[:, ni - 1], yu),
                (field.at[:, 0], yd),
            ]
            copy_all([pltpu.make_async_copy(a, b, sem.at[n]) for n, (a, b) in enumerate(pairs)])

        xau, xad, xbu, xbd, yu, yd = call(
            faces_body, [field_now],
            [vmem(xs)] * 4 + [vmem(ys)] * 2, [VM] * 6, [HBM],
            scratch=[pltpu.SemaphoreType.DMA((6,))], flops=1000, moved=6 * MIB,
        )

        def load_body(field, before, speed, now, prev, c, zu, zd, sem):
            copies = [
                pltpu.make_async_copy(field, now.at[:, :, pl.ds(PAD, nk)], sem.at[0]),
                pltpu.make_async_copy(before, prev.at[:, :, pl.ds(PAD, nk)], sem.at[1]),
                pltpu.make_async_copy(speed, c, sem.at[2]),
            ]
            for copy in copies:
                copy.start()
            copies[0].wait()
            z_faces(now, zu, zd)
            copies[1].wait()
            copies[2].wait()

        def z_faces(ref, zu, zd):
            def one(j, carry):
                for i in range(ni):
                    zd[j, pl.ds(i, 1), :] = ref[j, i, pl.ds(PAD, 1), :]
                    zu[j, pl.ds(i, 1), :] = ref[j, i, pl.ds(PAD + nk - 1, 1), :]
                return carry

            lax.fori_loop(0, nj, one, 0)

        now, prev, c, zu, zd = call(
            load_body, [field_now, earlier, speed_square],
            [vmem(padded), vmem(padded), vmem(field_now.shape), vmem(zs), vmem(zs)],
            [VM] * 5, [HBM] * 3,
            scratch=[pltpu.SemaphoreType.DMA((3,))], flops=40000000, moved=48 * MIB,
        )

        def row_ends(now, j, i, y_low, y_high):
            low = face(y_low, j) if isinstance(i, int) and i == 0 else inside(now, j, i - 1)
            high = face(y_high, j) if isinstance(i, int) and i == ni - 1 else inside(now, j, i + 1)
            return low, high

        def j_ends(now, j, i, x_low, x_high, first):
            if isinstance(j, int) and j == 0:
                return face(x_low, i - first), inside(now, 1, i)
            if isinstance(j, int) and j == nj - 1:
                return inside(now, nj - 2, i), face(x_high, i - first)
            return inside(now, j - 1, i), inside(now, j + 1, i)

        def edge_body(part):
            first = part * half
            outer = 0 if part == 0 else ni - 1
            inner = range(1, half) if part == 0 else range(half, ni - 1)

            def body(*refs):
                if part == 0:
                    now, before, speed, x_low, x_high, y_face, z_low, z_high = refs[:8]
                    now_out, out, xu, xd, yo = refs[8:]

                    def pads(j, carry):
                        for i in range(ni):
                            now_out[j, i, pl.ds(PAD - 1, 1), :] = z_low[j, pl.ds(i, 1), :]
                            now_out[j, i, pl.ds(PAD + nk, 1), :] = z_high[j, pl.ds(i, 1), :]
                        return carry

                    lax.fori_loop(0, nj, pads, 0)
                    now = now_out
                else:
                    now, before, speed, x_low, x_high, y_face = refs[:6]
                    out, xu, xd, yo = refs[6:]
                for j, x_out in ((0, xd), (nj - 1, xu)):
                    low, high = row_ends(now, j, outer, y_face, y_face)
                    columns(now, out, speed, j, outer, low, high, j_ends(now, j, outer, x_low, x_high, first),
                            [(x_out, outer - first), (yo, j)])

                    def one(i, carry, j=j, x_out=x_out):
                        low, high = row_ends(now, j, i, None, None)
                        columns(now, out, speed, j, i, low, high, j_ends(now, j, i, x_low, x_high, first),
                                [(x_out, i - first)])
                        return carry

                    lax.fori_loop(inner.start, inner.stop, one, 0)

                def side(j, carry):
                    low, high = row_ends(now, j, outer, y_face, y_face)
                    columns(now, out, speed, j, outer, low, high, j_ends(now, j, outer, None, None, first), [(yo, j)])
                    return carry

                lax.fori_loop(1, nj - 1, side, 0)

            return body

        def bulk_body(part):
            inner = range(1, half) if part == 0 else range(half, ni - 1)
            count = len(inner)

            def body(*refs):
                now, _, speed, out = refs[:4]

                def one(n, carry):
                    j, i = 1 + n // count, inner.start + n % count
                    low, high = row_ends(now, j, i, None, None)
                    columns(now, out, speed, j, i, low, high, j_ends(now, j, i, None, None, 0), [])
                    return carry

                lax.fori_loop(0, (nj - 2) * count, one, 0)
                if part == 1:
                    z_faces(out, *refs[4:])

            return body

        def last_body(part):
            first = part * half

            def body(*refs):
                if part == 0:
                    now, before, speed, x_low, x_high, y_face, z_low, z_high = refs[:8]
                    now_out, out, total = refs[8:]

                    def pads(j, carry):
                        for i in range(ni):
                            now_out[j, i, pl.ds(PAD - 1, 1), :] = z_low[j, pl.ds(i, 1), :]
                            now_out[j, i, pl.ds(PAD + nk, 1), :] = z_high[j, pl.ds(i, 1), :]
                        return carry

                    lax.fori_loop(0, nj, pads, 0)
                    now = now_out
                else:
                    now, before, speed, x_low, x_high, y_face = refs[:6]
                    out, total = refs[6:]

                def row(i):
                    for k in range(0, nk, ROWS):
                        acc = None
                        for j in range(nj):
                            low, high = row_ends(now, j, i, y_face, y_face)
                            jm, jp = j_ends(now, j, i, x_low, x_high, first)
                            new = cell_rows(now, out, speed, j, i, k, jm, jp, low, high)
                            out[j, i, pl.ds(PAD + k, ROWS), :] = new
                            acc = new if acc is None else acc + new
                        total[i - first, pl.ds(k, ROWS), :] = acc

                def one(i, carry):
                    row(i)
                    return carry

                if part == 0:
                    row(0)
                    lax.fori_loop(1, half, one, 0)
                else:
                    lax.fori_loop(half, ni - 1, one, 0)
                    row(ni - 1)

            return body

        def running_body(part):
            first = part * half
            scale = 1.0 / (nj * south)

            def body(*refs):
                u, p, q, r = refs[:4]
                result, buffer, sem = refs[-3:]

                def copy(i):
                    return pltpu.make_async_copy(buffer.at[:, i], result.at[:, first + i], sem)

                def one(i, carry):
                    for k in range(0, nk, ROWS):
                        rows = pl.ds(k, ROWS)
                        acc = p[i, rows, :] + q[i, rows, :] + r[i, rows, :]
                        for j in range(nj):
                            acc = acc + u[j, first + i, pl.ds(PAD + k, ROWS), :]
                            buffer[j, i, rows, :] = acc * scale
                    copy(i).start()
                    return carry

                lax.fori_loop(0, half, one, 0)
                pltpu.make_async_copy(buffer, result.at[:, pl.ds(first, half)], sem).wait()

            return body

        def store_body(u, result, sem):
            copy_all([pltpu.make_async_copy(u.at[:, :, pl.ds(PAD, nk)], result, sem)])

        a_low, a_high = send(xau, "south", south, 1), send(xad, "south", south, -1)
        y_low, y_high = send(yu, "east", east, 1), send(yd, "east", east, -1)
        b_low, b_high = send(xbu, "south", south, 1), send(xbd, "south", south, -1)
        z_low, z_high = send(zu, "down", down, 1), send(zd, "down", down, -1)

        for _ in range(STEPS - 1):
            now, prev, xau, xad, yd = call(
                edge_body(0),
                [now, prev, c, a_low, a_high, y_low, z_low, z_high],
                [vmem(padded), vmem(padded), vmem(xs), vmem(xs), vmem(ys)], [VM] * 5, [VM] * 8,
                alias={0: 0, 1: 1}, flops=3 * cells, moved=3 * MIB,
            )
            a_low, a_high = send(xau, "south", south, 1), send(xad, "south", south, -1)
            new_y_high = send(yd, "east", east, -1)
            prev = call(
                bulk_body(0), [now, prev, c], vmem(padded), VM, [VM] * 3,
                alias={1: 0}, flops=9 * cells, moved=8 * MIB,
            )
            prev, xbu, xbd, yu = call(
                edge_body(1),
                [now, prev, c, b_low, b_high, y_high],
                [vmem(padded), vmem(xs), vmem(xs), vmem(ys)], [VM] * 4, [VM] * 6,
                alias={1: 0}, flops=3 * cells, moved=3 * MIB,
            )
            y_low = send(yu, "east", east, 1)
            b_low, b_high = send(xbu, "south", south, 1), send(xbd, "south", south, -1)
            prev, zu, zd = call(
                bulk_body(1), [now, prev, c],
                [vmem(padded), vmem(zs), vmem(zs)], [VM] * 3, [VM] * 3,
                alias={1: 0}, flops=9 * cells, moved=8 * MIB,
            )
            z_low, z_high = send(zu, "down", down, 1), send(zd, "down", down, -1)
            y_high = new_y_high
            now, prev = prev, now

        def first_round(total):
            p = lax.ppermute(total, "south", [(0, 1), (1, 2)])
            return p, lax.ppermute(total, "south", [(0, 3)])

        def second_round(total, p, q):
            def body(total, p, q, out):
                last = lax.axis_index("south") == 3
                for i in range(half):
                    out[i] = jnp.where(last, q[i], total[i] + p[i])

            value = call(body, [total, p, q], vmem(xs), VM, [VM] * 3, flops=half * nk * nm, moved=2 * MIB)
            return lax.ppermute(value, "south", [(2, 3), (3, 2)])

        now, prev, total_a = call(
            last_body(0), [now, prev, c, a_low, a_high, y_low, z_low, z_high],
            [vmem(padded), vmem(padded), vmem(xs)], [VM] * 3, [VM] * 8,
            alias={0: 0, 1: 1}, flops=12 * cells, moved=12 * MIB,
        )
        pa, qa = first_round(total_a)
        prev, total_b = call(
            last_body(1), [now, prev, c, b_low, b_high, y_high],
            [vmem(padded), vmem(xs)], [VM] * 2, [VM] * 6,
            alias={1: 0}, flops=12 * cells, moved=12 * MIB,
        )
        pb, qb = first_round(total_b)
        end = call(
            store_body, [prev], jax.ShapeDtypeStruct(field_now.shape, jnp.float32), HBM, [VM],
            scratch=[pltpu.SemaphoreType.DMA], flops=10000000, moved=16 * MIB,
        )
        ra = second_round(total_a, pa, qa)
        rb = second_round(total_b, pb, qb)
        shape = jax.ShapeDtypeStruct(field_now.shape, jnp.float32)
        scratch = [pltpu.VMEM((nj, half, nk, nm), jnp.float32), pltpu.SemaphoreType.DMA]
        running = call(
            running_body(0), [prev, pa, qa, ra], shape, HBM, [VM] * 4,
            scratch=scratch, limit=10, flops=2 * cells, moved=8 * MIB,
        )
        running = call(
            running_body(1), [prev, pb, qb, rb, running], shape, HBM, [VM] * 4 + [HBM],
            alias={4: 0}, scratch=scratch, limit=10, flops=2 * cells, moved=8 * MIB,
        )
        return running, end

    spec = P("south", "east", "down", None)
    return jax.shard_map(shards, mesh=mesh, in_specs=(spec,) * 3, out_specs=(spec, spec), check_vma=False)
```
